32 devices in a mesh: groups: 2 (over y), dp: 4 (over z), section: 2 (over x), tensor: 2 (over core).
Axes of the slice: x: 2, y: 2, z: 4, core: 2. Of those that a mesh axis runs over, the one named last changes fastest.
Arguments:
- hidden: bfloat16 [128, 8, 5120], P(('groups', 'dp')), parts along dimension 0, may hold values from -6 to 6
- unembed: bfloat16 [128, 8, 5120], P(('groups', 'dp')), parts along dimension 0, may hold values from -0.02734375 to 0.02734375
- value_proj: bfloat16 [2, 5120, 512], P('section', 'dp', 'tensor'), may hold values from -0.078125 to 0.078125
- output_proj: bfloat16 [2, 512, 5120], P('section', 'tensor', 'dp'), may hold values from -0.125 to 0.125
- norm_gains: float32 [2, 5120], P('section'), may hold values from 0.1 to 1.9
- survive: int32 [8], P(('groups', 'dp')), parts along dimension 0, may hold values from 0 to 1, as said below
- lengths: int32 [128], P(('groups', 'dp')), parts along dimension 0, may hold values from 1 to 8
- assign: int32 [128], P(('groups', 'dp')), parts along dimension 0, may hold values from 0 to 16, as said below
- advantage: float32 [128], P(('groups', 'dp')), parts along dimension 0, may hold values from -4 to 4
- reference_logit: float32 [128, 8], P(('groups', 'dp')), parts along dimension 0, may hold values from -4 to 4
- recorded_gap: float32 [128, 8], P(('groups', 'dp')), parts along dimension 0, may hold values from -2 to 2
Outputs:
- grad_value: float32 [4, 5120, 512], P(('groups', 'section'), 'dp', 'tensor'), parts along dimension 0
- grad_output: float32 [4, 512, 5120], P(('groups', 'section'), 'tensor', 'dp'), parts along dimension 0
The draws below stay inside these ranges and needn't reach their ends.
There are 2 independent parts, one for each index of `groups`. The reference program is written for one: setup_inputs(seed, part) draws one part's arguments, and reference() takes and returns one part's arrays. A program takes and returns all parts, laid end to end along the dimension named above; an argument that names none is the same for every part. Nothing has to cross between parts.
Inputs may be any that keep to these rules, and one draw needn't show every extreme that they name: `survive`: 1 where the group of 16 responses is kept, 0 where it is dropped; in every draw all groups of some dp index are kept. `assign`: the 16 slots of a dp index list the local positions (0 to 15) of the responses of its kept groups, each exactly once, then hold 16 in every other slot.
All inputs are finite; a program needn't handle non-finite values.
Results may differ from the reference program's by a relative error of at most 0.029.
Values may be sent and summed in bfloat16 or wider, within the bound.
No kernel may reach another device: no remote copies, remote signals or barrier semaphores. Data moves between devices by JAX's collectives and lax.ppermute only.
A program may use at most 64 MiB of HBM per device.

```python
import math
import jax
import jax.numpy as jnp
from jax import lax

D = 5120
VALUE_W = 512
GROUP = 16
GROUPS_DEV = 1
LMAX = 8
LAYERS = 2
RESP_DEV = 16
RESPONSES = 64
GROUPS = 4
N_DP = 4
N_TENSOR = 2


def survival_plan(key):
    base = jax.random.fold_in(key, 17)
    roll_key, force_key, order_key = jax.random.split(base, 3)
    device = jnp.arange(GROUPS, dtype=jnp.int32) // GROUPS_DEV
    threshold = 300 + 700 * device // max(N_DP - 1, 1)
    survival_roll = jax.random.randint(roll_key, (GROUPS,), 0, 1000)
    forced = jax.random.randint(force_key, (), 0, N_DP)
    alive_mask = ((survival_roll < threshold) | (device == forced)).astype(jnp.int32)
    return (alive_mask, order_key)


def draw_survive(key, part):
    alive_mask, order_key = survival_plan(key)
    return alive_mask


def draw_assign(key, part):
    alive_mask, order_key = survival_plan(key)
    per_device = jnp.repeat(alive_mask, GROUP).reshape(N_DP, RESP_DEV)
    subkeys = jax.random.split(order_key, N_DP)
    priority = jax.vmap(lambda subkey: jax.random.permutation(subkey, RESP_DEV))(subkeys).astype(jnp.int32)
    sort_key = (1 - per_device) * RESP_DEV + priority
    slot_order = jnp.argsort(sort_key, axis=1, stable=True).astype(jnp.int32)
    alive_count = jnp.sum(per_device, axis=1, keepdims=True)
    slot_index = lax.broadcasted_iota(jnp.int32, (N_DP, RESP_DEV), 1)
    return jnp.where(slot_index < alive_count, slot_order, RESP_DEV).astype(jnp.int32).reshape(RESPONSES)


def set_ends(drawn, rng, low, high):
    extent = drawn.shape
    spot = [jax.random.randint(jax.random.fold_in(rng, axis), (), 0, extent[axis]) for axis in range(len(extent))]
    drawn = drawn.at[tuple(spot)].set(low)
    longest = extent.index(max(extent))
    spot[longest] = (spot[longest] + 1) % extent[longest]
    return drawn.at[tuple(spot)].set(high)


def with_spikes(values, rng, source, target, parts, factor):
    owner, partner = [(jnp.arange(values.shape[axis_at]) // (values.shape[axis_at] // parts)).reshape([-1 if axis == axis_at else 1 for axis in range(values.ndim)]) for axis_at in (source, target)]
    chosen = jax.random.permutation(rng, parts)[partner]
    strong = (owner == chosen) | (owner == (partner + parts // 2) % parts)
    return jnp.where(strong, factor * values, values)


def shard_levels(own_key, shape, cuts, least, top_value):
    gain, own = 1.0, jax.random.fold_in(own_key, 6)
    for position, parts in cuts:
        heights = jnp.exp(jax.random.uniform(jax.random.fold_in(own, position), (parts,), jnp.float32, least / len(cuts), top_value / len(cuts)))
        gain = gain * jnp.repeat(heights, shape[position] // parts).reshape([-1 if axis == position else 1 for axis in range(len(shape))])
    return gain


def normal_values(own_key, dims, scale, limit, cuts=(), held_as=jnp.bfloat16):
    result = jax.random.normal(own_key, dims, jnp.float32) * scale
    if len(cuts) > 0:
        result = shard_levels(own_key, dims, cuts, -0.22, 0.18) * result
    return jnp.clip(result, min=-limit, max=limit).astype(held_as)


def heavy_noise(key, shape, scale, most, cuts, heavy, held_as=jnp.bfloat16):
    entries = scale * jax.random.normal(key, shape, jnp.float32)
    if cuts:
        entries = entries * shard_levels(key, shape, cuts, -0.22, 0.18)
    return jnp.clip(with_spikes(entries, jax.random.fold_in(key, 3), *heavy), -most, most).astype(held_as)


def setup_inputs(seed: int = 0, part: int = 0) -> dict:
    key_list = jax.random.split(jax.random.key(seed), 12)
    own_keys = jax.random.split(jax.random.fold_in(key_list[11], part), 12)
    return {
        "hidden": heavy_noise(own_keys[0], (RESPONSES, LMAX, D), 1.0, 6.0, ((0, 4),), (0, 2, 4, 2.0)),
        "unembed": normal_values(own_keys[1], (RESPONSES, LMAX, D), (10 * D) ** -0.5, 0.02734375, ((0, 4),)),
        "value_proj": normal_values(key_list[2], (LAYERS, D, VALUE_W), D ** -0.5, 0.078125, ((0, 2), (1, 4), (2, 2))),
        "output_proj": normal_values(key_list[3], (LAYERS, VALUE_W, D), (4 * VALUE_W) ** -0.5, 0.125, ((0, 2), (1, 2), (2, 4))),
        "norm_gains": jnp.clip(1.0 + 0.18 * jax.random.normal(key_list[4], (LAYERS, D), jnp.float32), 0.1, 1.9),
        "survive": draw_survive(jax.random.fold_in(jax.random.fold_in(key_list[11], part), 71), part),
        "lengths": set_ends(jax.random.randint(own_keys[6], (RESPONSES,), 1, LMAX + 1), jax.random.fold_in(own_keys[6], 1), 1, LMAX).astype(jnp.int32),
        "assign": draw_assign(jax.random.fold_in(jax.random.fold_in(key_list[11], part), 71), part),
        "advantage": normal_values(own_keys[8], (RESPONSES,), 1.0, 4.0, ((0, 4),), jnp.float32),
        "reference_logit": normal_values(own_keys[9], (RESPONSES, LMAX), 0.7, 4.0, ((0, 4),), jnp.float32),
        "recorded_gap": normal_values(own_keys[10], (RESPONSES, LMAX), 0.3, 2.0, ((0, 4),), jnp.float32),
    }


eps_norm = 1e-06
loss_scale = 4096.0
clip_high = math.log(1.28)
clip_low = math.log(0.8)

def norm_forward(row_block, norm_gain):
    values = row_block.astype(jnp.float32)
    inverse = lax.rsqrt(lax.optimization_barrier(jnp.mean(values * values, axis=-1, keepdims=True)) + eps_norm)
    return (values, inverse, (values * inverse * norm_gain).astype(jnp.bfloat16))

def norm_backward(values, inverse, norm_gain, upstream):
    scaled = upstream * norm_gain
    inner_sum = lax.optimization_barrier(jnp.sum(scaled * values, axis=-1, keepdims=True)) / values.shape[-1]
    return inverse * scaled - values * (inverse * inverse * inverse) * inner_sum

def contract_last(left_rows, right_rows):
    return lax.dot_general(left_rows, right_rows, (((1,), (1,)), ((), ())), preferred_element_type=jnp.float32)

def rounded(partial_piece):
    return lax.optimization_barrier(partial_piece.astype(jnp.bfloat16)).astype(jnp.float32)

def reference(hidden, unembed, value_proj, output_proj, norm_gains, survive, lengths, assign, advantage, reference_logit, recorded_gap):
    owner_index = jnp.arange(RESPONSES, dtype=jnp.int32) // RESP_DEV
    chosen = jnp.where(assign >= RESP_DEV, RESPONSES, assign + owner_index * RESP_DEV).astype(jnp.int32)

    def pick(array):
        return jnp.take(array, chosen, axis=0, mode='fill', fill_value=0)
    row_count = RESPONSES * LMAX
    block_width = VALUE_W // N_TENSOR
    current = pick(hidden).reshape(row_count, D)
    unembed_rows = pick(unembed).reshape(row_count, D).astype(jnp.float32)
    positions = lax.broadcasted_iota(jnp.int32, (RESPONSES, LMAX), 1)
    live_mask = (positions < pick(lengths)[:, None]).astype(jnp.float32)
    advantages = jnp.broadcast_to(pick(advantage)[:, None], (RESPONSES, LMAX))
    gap_rows = pick(recorded_gap)
    clipped = (advantages > 0) & (gap_rows > clip_high) | (advantages < 0) & (gap_rows < clip_low)
    kept_mask = 1.0 - clipped.astype(jnp.float32)
    alive_mask = jnp.repeat(survive, GROUP)
    token_count = jnp.sum((alive_mask * lengths).astype(jnp.float32))
    weight_rows = (-loss_scale * advantages * kept_mask * live_mask).reshape(row_count)
    logit_base = pick(reference_logit).reshape(row_count)
    saved = []
    for layer_index in range(LAYERS):
        values, inverse, normed = norm_forward(current, norm_gains[layer_index])
        projected = jnp.dot(normed, value_proj[layer_index], preferred_element_type=jnp.float32).astype(jnp.bfloat16)
        mixed_sum = jnp.zeros((row_count, D), jnp.float32)
        for tensor_part in range(N_TENSOR):
            low = tensor_part * block_width
            partial_piece = jnp.dot(projected[:, low:low + block_width], output_proj[layer_index, low:low + block_width, :], preferred_element_type=jnp.float32)
            mixed_sum = mixed_sum + rounded(partial_piece)
        saved.append((current, normed, projected))
        current = (values + mixed_sum).astype(jnp.bfloat16)
    top_rows = current.astype(jnp.float32)
    logit = lax.optimization_barrier(jnp.sum(top_rows * unembed_rows, axis=-1))
    seed_rows = weight_rows * jnp.exp(logit - logit_base)
    upstream = (seed_rows[:, None] * unembed_rows).astype(jnp.bfloat16)
    grads_value = [None] * LAYERS
    grads_output = [None] * LAYERS
    for layer_index in reversed(range(LAYERS)):
        entering, normed, projected = saved[layer_index]
        grad_projected = contract_last(upstream, output_proj[layer_index]).astype(jnp.bfloat16)
        grad_normed = jnp.zeros((row_count, D), jnp.float32)
        for tensor_part in range(N_TENSOR):
            low = tensor_part * block_width
            partial_piece = contract_last(grad_projected[:, low:low + block_width], value_proj[layer_index][:, low:low + block_width])
            grad_normed = grad_normed + rounded(partial_piece)
        grads_value[layer_index] = jnp.dot(normed.T, grad_projected, preferred_element_type=jnp.float32) / token_count
        grads_output[layer_index] = jnp.dot(projected.T, upstream, preferred_element_type=jnp.float32) / token_count
        values, inverse, unused_normed = norm_forward(entering, norm_gains[layer_index])
        upstream = (upstream.astype(jnp.float32) + norm_backward(values, inverse, norm_gains[layer_index], grad_normed)).astype(jnp.bfloat16)
    return (jnp.stack(grads_value), jnp.stack(grads_output))
```

```python
import math

import jax
import jax.numpy as jnp
from jax import lax
from jax.sharding import PartitionSpec as P

GROUP = 16
MB_RESP = 8


eps_norm = 1e-06
loss_scale = 4096.0
clip_high = math.log(1.28)
clip_low = math.log(0.8)


def from_behind(block, axis, distance):
    devices = range(lax.axis_size(axis))
    route = [(i - distance, i) for i in devices if i - distance in devices]
    return lax.ppermute(block, axis, route)


def norm_forward(row_block, norm_gain):
    values = row_block.astype(jnp.float32)
    inverse = lax.rsqrt(jnp.mean(values * values, axis=-1, keepdims=True) + eps_norm)
    return (values, inverse, (values * inverse * norm_gain).astype(jnp.bfloat16))


def norm_backward(values, inverse, norm_gain, upstream):
    scaled = upstream * norm_gain
    inner_sum = jnp.sum(scaled * values, axis=-1, keepdims=True) / values.shape[-1]
    return inverse * scaled - values * (inverse * inverse * inverse) * inner_sum


def contract_last(left_rows, right_rows):
    return lax.dot_general(
        left_rows, right_rows, (((1,), (1,)), ((), ())), preferred_element_type=jnp.float32
    )


def contract_first(left_rows, right_rows):
    return lax.dot_general(
        left_rows, right_rows, (((0,), (0,)), ((), ())), preferred_element_type=jnp.float32
    )


def take_slot(slot_store, slot_index):
    return lax.dynamic_index_in_dim(slot_store, slot_index, 0, keepdims=False)


def put_slot(slot_store, new_value, slot_index, active):
    previous = take_slot(slot_store, slot_index)
    return lax.dynamic_update_index_in_dim(
        slot_store, jnp.where(active, new_value, previous), slot_index, 0
    )


def general(
    hidden,
    unembed,
    value_proj,
    output_proj,
    norm_gains,
    survive,
    lengths,
    assign,
    advantage,
    reference_logit,
    recorded_gap,
):
    resp_count = hidden.shape[0]
    positions = hidden.shape[1]
    model_width = hidden.shape[2]
    half_value = value_proj.shape[2]
    micro_count = resp_count // MB_RESP
    row_count = MB_RESP * positions
    section_count = lax.axis_size("section")
    section_index = lax.axis_index("section")
    is_last = section_index == section_count - 1
    norm_gain = norm_gains[0]
    alive_mask = jnp.repeat(survive, GROUP)
    local_count = jnp.sum((alive_mask * lengths).astype(jnp.float32))
    gathered_value, gathered_output = (
        lax.all_gather(value_proj, "dp", axis=1, tiled=True),
        lax.all_gather(output_proj, "dp", axis=2, tiled=True),
    )
    w_first = gathered_value[0]
    w_second = gathered_output[0]

    def pick(array):
        return jnp.take(array, assign, axis=0, mode="fill", fill_value=0)

    slot_hidden = pick(hidden).reshape(micro_count, row_count, model_width)
    slot_unembed = pick(unembed).reshape(micro_count, row_count, model_width)
    position_index = lax.broadcasted_iota(jnp.int32, (resp_count, positions), 1)
    live_mask = (position_index < pick(lengths)[:, None]).astype(jnp.float32)
    advantages = jnp.broadcast_to(pick(advantage)[:, None], (resp_count, positions))
    gap_rows = pick(recorded_gap)
    clipped = (advantages > 0) & (gap_rows > clip_high) | (advantages < 0) & (gap_rows < clip_low)
    kept_mask = 1.0 - clipped.astype(jnp.float32)
    weight_rows = (-loss_scale * advantages * kept_mask * live_mask).reshape(micro_count, row_count)
    logit_base = pick(reference_logit).reshape(micro_count, row_count)
    step_count = micro_count + section_count - 1
    store_in = jnp.zeros((micro_count, row_count, model_width), jnp.bfloat16)
    store_normed = jnp.zeros((micro_count, row_count, model_width), jnp.bfloat16)
    store_projected = jnp.zeros((micro_count, row_count, half_value), jnp.bfloat16)
    store_out = jnp.zeros((micro_count, row_count, model_width), jnp.bfloat16)
    arriving = jnp.zeros((row_count, model_width), jnp.bfloat16)
    for step_index in range(step_count):
        micro_index = step_index - section_index
        active = (micro_index >= 0) & (micro_index < micro_count)
        clamped = jnp.clip(micro_index, 0, micro_count - 1)
        entering = jnp.where(section_index == 0, take_slot(slot_hidden, clamped), arriving)
        values, inverse, normed = norm_forward(entering, norm_gain)
        projected = jnp.dot(normed, w_first, preferred_element_type=jnp.float32).astype(
            jnp.bfloat16
        )
        partial_out = jnp.dot(projected, w_second, preferred_element_type=jnp.float32)
        mixed_sum = lax.psum(partial_out.astype(jnp.bfloat16), "tensor").astype(jnp.float32)
        leaving = (values + mixed_sum).astype(jnp.bfloat16)
        store_in = put_slot(store_in, entering, clamped, active)
        store_normed = put_slot(store_normed, normed, clamped, active)
        store_projected = put_slot(store_projected, projected, clamped, active)
        store_out = put_slot(store_out, leaving, clamped, active)
        arriving = from_behind(leaving, "section", 1)
    store_upstream = jnp.zeros((micro_count, row_count, model_width), jnp.bfloat16)
    store_grad_value = jnp.zeros((micro_count, row_count, half_value), jnp.bfloat16)
    arriving = jnp.zeros((row_count, model_width), jnp.bfloat16)
    for step_index in range(step_count):
        micro_index = step_index - (section_count - 1 - section_index)
        active = (micro_index >= 0) & (micro_index < micro_count)
        clamped = jnp.clip(micro_index, 0, micro_count - 1)
        top_rows = take_slot(store_out, clamped).astype(jnp.float32)
        unembed_rows = take_slot(slot_unembed, clamped).astype(jnp.float32)
        logit = jnp.sum(top_rows * unembed_rows, axis=-1)
        seed_rows = take_slot(weight_rows, clamped) * jnp.exp(
            logit - take_slot(logit_base, clamped)
        )
        start_grad = (seed_rows[:, None] * unembed_rows).astype(jnp.bfloat16)
        upstream = jnp.where(is_last, start_grad, arriving)
        entering = take_slot(store_in, clamped)
        normed = take_slot(store_normed, clamped)
        projected = take_slot(store_projected, clamped)
        grad_projected = contract_last(upstream, w_second).astype(jnp.bfloat16)
        partial_norm = contract_last(grad_projected, w_first)
        grad_normed = lax.psum(partial_norm.astype(jnp.bfloat16), "tensor").astype(jnp.float32)
        values, inverse, unused_normed = norm_forward(entering, norm_gain)
        grad_entering = (
            upstream.astype(jnp.float32) + norm_backward(values, inverse, norm_gain, grad_normed)
        ).astype(jnp.bfloat16)
        store_upstream = put_slot(store_upstream, upstream, clamped, active)
        store_grad_value = put_slot(store_grad_value, grad_projected, clamped, active)
        arriving = from_behind(grad_entering, "section", -1)
    flat_normed = store_normed.reshape(micro_count * row_count, model_width)
    flat_upstream = store_upstream.reshape(micro_count * row_count, model_width)
    flat_grad_value = store_grad_value.reshape(micro_count * row_count, half_value)
    flat_projected = store_projected.reshape(micro_count * row_count, half_value)
    reduced = lax.psum_scatter(
        jnp.concatenate(
            [
                contract_first(flat_normed, flat_grad_value),
                contract_first(flat_upstream, flat_projected),
            ],
            axis=1,
        ).astype(jnp.bfloat16),
        "dp",
        scatter_dimension=0,
        tiled=True,
    ).astype(jnp.float32)
    token_total = lax.psum(local_count, "dp")
    scaled_grads = reduced / token_total
    grad_value = scaled_grads[:, :half_value][None]
    grad_output = scaled_grads[:, half_value:].T[None]
    return (grad_value, grad_output)


def rotate(block, axis, distance):
    count = lax.axis_size(axis)
    return lax.ppermute(block, axis, [(i, (i + distance) % count) for i in range(count)])


def swap(block, axis):
    return rotate(block, axis, 1)


def low_rank(
    hidden,
    unembed,
    value_proj,
    output_proj,
    norm_gains,
    survive,
    lengths,
    assign,
    advantage,
    reference_logit,
    recorded_gap,
):
    f32, bf16 = jnp.float32, jnp.bfloat16
    resp_count, positions, model_width = hidden.shape
    _, own_width, half_value = value_proj.shape
    dp_count, group_count = lax.axis_size("dp"), lax.axis_size("groups")
    dp_index, group_index = lax.axis_index("dp"), lax.axis_index("groups")
    tensor_index = lax.axis_index("tensor")
    first = lax.axis_index("section") == 0
    half_resp = resp_count // 2
    half_rows = half_resp * positions
    shifts = range(1, dp_count)

    def my_half(array):
        return lax.dynamic_slice_in_dim(array, tensor_index * half_resp, half_resp, 0)

    def columns(array, index):
        return lax.dynamic_slice_in_dim(array, index * own_width, own_width, array.ndim - 1)

    gain = columns(norm_gains[0], dp_index)
    a_own = (value_proj[0].astype(f32) * gain[:, None]).astype(bf16).T
    b_own = output_proj[0]
    hid_half = my_half(hidden).reshape(half_rows, model_width)
    un_half = my_half(unembed).reshape(half_rows, model_width)
    moved = jnp.where(first, hid_half, un_half)
    arrived = [columns(moved, dp_index)]
    for d in shifts:
        arrived.append(rotate(columns(moved, (dp_index + d) % dp_count), "dp", d))
    c_own = swap(jnp.where(first, b_own, a_own), "section")
    ab_other = swap(jnp.concatenate([a_own, b_own]), "tensor")
    a_all = jnp.concatenate([a_own, ab_other[:half_value]])
    b_all = jnp.concatenate([b_own, ab_other[half_value:]])
    c_all = jnp.concatenate([c_own, swap(c_own, "tensor")])

    part_rows = half_value // group_count
    block_rows = part_rows // dp_count
    left = lax.dynamic_slice_in_dim(
        jnp.where(first, b_own, c_own), group_index * part_rows, part_rows, 0
    )
    part = contract_last(left, jnp.where(first, b_all, a_all))

    def part_block(index):
        return lax.dynamic_slice_in_dim(part, index * block_rows, block_rows, 0)

    total = part_block(dp_index)
    for d in shifts:
        total = total + rotate(
            part_block((dp_index + d) % dp_count).astype(bf16), "dp", d
        ).astype(f32)
    total = total.astype(bf16)
    product = jnp.zeros((part_rows, 2 * half_value), bf16)
    product = lax.dynamic_update_slice_in_dim(product, total, dp_index * block_rows, 0)
    for d in shifts:
        product = lax.dynamic_update_slice_in_dim(
            product, rotate(total, "dp", d), (dp_index - d) % dp_count * block_rows, 0
        )
    grown = jnp.zeros((half_value, 2 * half_value), bf16)
    grown = lax.dynamic_update_slice_in_dim(grown, product, group_index * part_rows, 0)
    for d in range(1, group_count):
        grown = lax.dynamic_update_slice_in_dim(
            grown,
            rotate(product, "groups", d),
            (group_index - d) % group_count * part_rows,
            0,
        )
    across = swap(grown, "section")
    both = jnp.concatenate([jnp.where(first, grown, across), jnp.where(first, across, grown)])
    both_other = swap(both, "tensor")
    both_other = jnp.concatenate([both_other[:, half_value:], both_other[:, :half_value]], axis=1)
    gram = jnp.concatenate([both[:half_value], both_other[:half_value]])
    link = jnp.concatenate([both[half_value:], both_other[half_value:]])

    rows_here = jnp.concatenate(arrived)
    weights = jnp.concatenate([a_all, b_all, c_all])
    partial = contract_last(rows_here, weights)
    summed = partial[:half_rows]
    for d in shifts:
        block = partial[d * half_rows : (d + 1) * half_rows].astype(bf16)
        summed = summed + rotate(block, "dp", -d).astype(f32)
    mine = summed.astype(bf16)
    theirs = swap(mine, "section")
    from_hidden = jnp.where(first, mine, theirs).astype(f32)
    from_unembed = jnp.where(first, theirs, mine).astype(f32)
    width = 2 * half_value
    a0, b0, a1 = (from_hidden[:, i * width : (i + 1) * width] for i in range(3))
    t1, t0 = (from_unembed[:, i * width : (i + 1) * width] for i in range(1, 3))

    local_count = jnp.sum(
        (jnp.repeat(survive, resp_count // survive.shape[0]) * lengths).astype(f32)
    )
    listed = jnp.any(assign[None, :] == jnp.arange(resp_count)[:, None], axis=1)
    position_index = lax.broadcasted_iota(jnp.int32, (half_resp, positions), 1)
    live = (position_index < my_half(lengths)[:, None]) & my_half(listed)[:, None]
    adv = my_half(advantage)[:, None]
    gap = my_half(recorded_gap)
    clipped = (adv > 0) & (gap > clip_high) | (adv < 0) & (gap < clip_low)
    weight = jnp.where(live & ~clipped, -loss_scale * adv, 0.0).reshape(half_rows, 1)
    base = my_half(reference_logit).reshape(half_rows, 1)
    listed_rows = jnp.repeat(my_half(listed), positions)[:, None]
    hid32, un32 = hid_half.astype(f32), un_half.astype(f32)

    def row_sum(array):
        return jnp.sum(array, axis=-1, keepdims=True)

    square0 = row_sum(hid32 * hid32)
    dot0 = row_sum(hid32 * un32)
    r0 = lax.rsqrt(square0 / model_width + eps_norm)
    p0b = (r0 * a0).astype(bf16)
    p0 = p0b.astype(f32)
    linked = jnp.dot(p0b, link, preferred_element_type=f32)
    grammed = jnp.dot(p0b, gram, preferred_element_type=f32)
    square1 = square0 + row_sum(p0 * (2.0 * b0 + grammed))
    r1 = lax.rsqrt(jnp.maximum(square1, 0.0) / model_width + eps_norm)
    p1 = r1 * (a1 + linked)
    logit = dot0 + row_sum(p0 * t0) + row_sum(p1 * t1)
    seed = weight * jnp.exp(jnp.where(listed_rows, logit - base, 0.0))
    gp1 = seed * t1
    c1 = r1 * r1 * row_sum(gp1 * p1) / model_width
    back = contract_last(gp1.astype(bf16), link)
    gp0 = seed * t0 + r1 * back - c1 * (b0 + grammed)

    early = jnp.where(first, p0b, mine[:, width : 2 * width])
    early_all = jnp.concatenate([early] + [rotate(early, "dp", d) for d in shifts])
    early_cross = swap(early_all, "section")
    early_two = jnp.concatenate([early_all, early_cross], axis=1)
    early_rows = jnp.concatenate([early_two, swap_columns(swap(early_two, "tensor"), half_value)])
    p0_rows = jnp.where(first, early_rows[:, :width], early_rows[:, width:])
    t1_rows = jnp.where(first, early_rows[:, width:], early_rows[:, :width])

    here_cross = swap(rows_here, "section")
    here_two = jnp.concatenate([rows_here, here_cross], axis=1)
    here_rows = jnp.concatenate([here_two, swap(here_two, "tensor")])
    hid_rows = jnp.where(first, here_rows[:, :own_width], here_rows[:, own_width:])
    un_rows = jnp.where(first, here_rows[:, own_width:], here_rows[:, :own_width])

    late = jnp.where(first, r0 * gp0, seed * p1).astype(bf16)
    scalars = jnp.concatenate([seed, r1, c1, jnp.full_like(seed, local_count)], axis=1)
    high = lax.reduce_precision(scalars, 8, 7)
    extra = jnp.concatenate([high, scalars - high], axis=1).astype(bf16)
    extra = jnp.pad(extra, ((0, 0), (0, 128 - extra.shape[1])))
    late_own = jnp.concatenate([late[:, :half_value], extra], axis=1)
    late_other = swap(jnp.concatenate([late[:, half_value:], extra], axis=1), "tensor")
    late_here = jnp.concatenate([late_own, late_other])
    pieces = [late_here] + [rotate(late_here, "dp", d) for d in shifts]
    late_rows = jnp.concatenate([p[:half_rows] for p in pieces] + [p[half_rows:] for p in pieces])
    found = late_rows[:, half_value : half_value + 8].astype(f32)
    found = found[:, :4] + found[:, 4:]
    seed_rows, r1_rows, c1_rows = found[:, 0:1], found[:, 1:2], found[:, 2:3]
    token_total = jnp.sum(found[:: half_rows, 3]) / 2.0
    late_rows = late_rows[:, :half_value]

    hid32_rows = hid_rows.astype(f32)
    x1_rows = hid32_rows + jnp.dot(
        p0_rows, jnp.where(first, b_all, c_all), preferred_element_type=f32
    )
    n1_rows = jnp.dot(t1_rows, c_all, preferred_element_type=f32)
    g1_rows = seed_rows * (un_rows.astype(f32) + r1_rows * n1_rows) - c1_rows * x1_rows
    value_left = jnp.where(
        first, late_rows, (seed_rows * r1_rows * t1_rows[:, :half_value].astype(f32)).astype(bf16)
    )
    value_right = jnp.where(first, hid_rows, x1_rows.astype(bf16))
    output_left = jnp.where(first, p0_rows[:, :half_value], late_rows)
    output_right = jnp.where(first, g1_rows.astype(bf16), un_rows)
    grad_value = contract_first(value_right, value_left) * (gain[:, None] / token_total)
    grad_output = contract_first(output_left, output_right) / token_total
    return (grad_value[None], grad_output[None])


def swap_columns(array, half_value):
    low, high = array[:, :half_value], array[:, half_value : 2 * half_value]
    low2, high2 = array[:, 2 * half_value : 3 * half_value], array[:, 3 * half_value :]
    return jnp.concatenate([high, low, high2, low2], axis=1)


def solution(mesh):
    placed = (
        P(("groups", "dp"), None, None),
        P(("groups", "dp"), None, None),
        P("section", "dp", "tensor"),
        P("section", "tensor", "dp"),
        P("section", None),
        P(("groups", "dp")),
        P(("groups", "dp")),
        P(("groups", "dp")),
        P(("groups", "dp")),
        P(("groups", "dp"), None),
        P(("groups", "dp"), None),
    )
    two_by_two = mesh.shape["section"] == 2 and mesh.shape["tensor"] == 2
    return jax.shard_map(
        low_rank if two_by_two else general,
        mesh=mesh,
        in_specs=placed,
        out_specs=(
            P(("groups", "section"), "dp", "tensor"),
            P(("groups", "section"), "tensor", "dp"),
        ),
        check_vma=False,
    )
```

```python
import functools
import math

import jax
import jax.numpy as jnp
from jax import lax
from jax.experimental import pallas as pl
from jax.experimental.pallas import tpu as pltpu
from jax.sharding import PartitionSpec as P


GROUP = 16
MB_RESP = 8


eps_norm = 1e-06
loss_scale = 4096.0
clip_high = math.log(1.28)
clip_low = math.log(0.8)


def from_behind(block, axis, distance):
    devices = range(lax.axis_size(axis))
    route = [(i - distance, i) for i in devices if i - distance in devices]
    return lax.ppermute(block, axis, route)


def norm_forward(row_block, norm_gain):
    values = row_block.astype(jnp.float32)
    inverse = lax.rsqrt(jnp.mean(values * values, axis=-1, keepdims=True) + eps_norm)
    return (values, inverse, (values * inverse * norm_gain).astype(jnp.bfloat16))


def norm_backward(values, inverse, norm_gain, upstream):
    scaled = upstream * norm_gain
    inner_sum = jnp.sum(scaled * values, axis=-1, keepdims=True) / values.shape[-1]
    return inverse * scaled - values * (inverse * inverse * inverse) * inner_sum


def contract_last(left_rows, right_rows):
    return lax.dot_general(
        left_rows, right_rows, (((1,), (1,)), ((), ())), preferred_element_type=jnp.float32
    )


def contract_first(left_rows, right_rows):
    return lax.dot_general(
        left_rows, right_rows, (((0,), (0,)), ((), ())), preferred_element_type=jnp.float32
    )


def take_slot(slot_store, slot_index):
    return lax.dynamic_index_in_dim(slot_store, slot_index, 0, keepdims=False)


def put_slot(slot_store, new_value, slot_index, active):
    previous = take_slot(slot_store, slot_index)
    return lax.dynamic_update_index_in_dim(
        slot_store, jnp.where(active, new_value, previous), slot_index, 0
    )


def general(
    hidden,
    unembed,
    value_proj,
    output_proj,
    norm_gains,
    survive,
    lengths,
    assign,
    advantage,
    reference_logit,
    recorded_gap,
):
    resp_count = hidden.shape[0]
    positions = hidden.shape[1]
    model_width = hidden.shape[2]
    half_value = value_proj.shape[2]
    micro_count = resp_count // MB_RESP
    row_count = MB_RESP * positions
    section_count = lax.axis_size("section")
    section_index = lax.axis_index("section")
    is_last = section_index == section_count - 1
    norm_gain = norm_gains[0]
    alive_mask = jnp.repeat(survive, GROUP)
    local_count = jnp.sum((alive_mask * lengths).astype(jnp.float32))
    gathered_value, gathered_output = (
        lax.all_gather(value_proj, "dp", axis=1, tiled=True),
        lax.all_gather(output_proj, "dp", axis=2, tiled=True),
    )
    w_first = gathered_value[0]
    w_second = gathered_output[0]

    def pick(array):
        return jnp.take(array, assign, axis=0, mode="fill", fill_value=0)

    slot_hidden = pick(hidden).reshape(micro_count, row_count, model_width)
    slot_unembed = pick(unembed).reshape(micro_count, row_count, model_width)
    position_index = lax.broadcasted_iota(jnp.int32, (resp_count, positions), 1)
    live_mask = (position_index < pick(lengths)[:, None]).astype(jnp.float32)
    advantages = jnp.broadcast_to(pick(advantage)[:, None], (resp_count, positions))
    gap_rows = pick(recorded_gap)
    clipped = (advantages > 0) & (gap_rows > clip_high) | (advantages < 0) & (gap_rows < clip_low)
    kept_mask = 1.0 - clipped.astype(jnp.float32)
    weight_rows = (-loss_scale * advantages * kept_mask * live_mask).reshape(micro_count, row_count)
    logit_base = pick(reference_logit).reshape(micro_count, row_count)
    step_count = micro_count + section_count - 1
    store_in = jnp.zeros((micro_count, row_count, model_width), jnp.bfloat16)
    store_normed = jnp.zeros((micro_count, row_count, model_width), jnp.bfloat16)
    store_projected = jnp.zeros((micro_count, row_count, half_value), jnp.bfloat16)
    store_out = jnp.zeros((micro_count, row_count, model_width), jnp.bfloat16)
    arriving = jnp.zeros((row_count, model_width), jnp.bfloat16)
    for step_index in range(step_count):
        micro_index = step_index - section_index
        active = (micro_index >= 0) & (micro_index < micro_count)
        clamped = jnp.clip(micro_index, 0, micro_count - 1)
        entering = jnp.where(section_index == 0, take_slot(slot_hidden, clamped), arriving)
        values, inverse, normed = norm_forward(entering, norm_gain)
        projected = jnp.dot(normed, w_first, preferred_element_type=jnp.float32).astype(
            jnp.bfloat16
        )
        partial_out = jnp.dot(projected, w_second, preferred_element_type=jnp.float32)
        mixed_sum = lax.psum(partial_out.astype(jnp.bfloat16), "tensor").astype(jnp.float32)
        leaving = (values + mixed_sum).astype(jnp.bfloat16)
        store_in = put_slot(store_in, entering, clamped, active)
        store_normed = put_slot(store_normed, normed, clamped, active)
        store_projected = put_slot(store_projected, projected, clamped, active)
        store_out = put_slot(store_out, leaving, clamped, active)
        arriving = from_behind(leaving, "section", 1)
    store_upstream = jnp.zeros((micro_count, row_count, model_width), jnp.bfloat16)
    store_grad_value = jnp.zeros((micro_count, row_count, half_value), jnp.bfloat16)
    arriving = jnp.zeros((row_count, model_width), jnp.bfloat16)
    for step_index in range(step_count):
        micro_index = step_index - (section_count - 1 - section_index)
        active = (micro_index >= 0) & (micro_index < micro_count)
        clamped = jnp.clip(micro_index, 0, micro_count - 1)
        top_rows = take_slot(store_out, clamped).astype(jnp.float32)
        unembed_rows = take_slot(slot_unembed, clamped).astype(jnp.float32)
        logit = jnp.sum(top_rows * unembed_rows, axis=-1)
        seed_rows = take_slot(weight_rows, clamped) * jnp.exp(
            logit - take_slot(logit_base, clamped)
        )
        start_grad = (seed_rows[:, None] * unembed_rows).astype(jnp.bfloat16)
        upstream = jnp.where(is_last, start_grad, arriving)
        entering = take_slot(store_in, clamped)
        normed = take_slot(store_normed, clamped)
        projected = take_slot(store_projected, clamped)
        grad_projected = contract_last(upstream, w_second).astype(jnp.bfloat16)
        partial_norm = contract_last(grad_projected, w_first)
        grad_normed = lax.psum(partial_norm.astype(jnp.bfloat16), "tensor").astype(jnp.float32)
        values, inverse, _ = norm_forward(entering, norm_gain)
        grad_entering = (
            upstream.astype(jnp.float32) + norm_backward(values, inverse, norm_gain, grad_normed)
        ).astype(jnp.bfloat16)
        store_upstream = put_slot(store_upstream, upstream, clamped, active)
        store_grad_value = put_slot(store_grad_value, grad_projected, clamped, active)
        arriving = from_behind(grad_entering, "section", -1)
    flat_normed = store_normed.reshape(micro_count * row_count, model_width)
    flat_upstream = store_upstream.reshape(micro_count * row_count, model_width)
    flat_grad_value = store_grad_value.reshape(micro_count * row_count, half_value)
    flat_projected = store_projected.reshape(micro_count * row_count, half_value)
    reduced = lax.psum_scatter(
        jnp.concatenate(
            [
                contract_first(flat_normed, flat_grad_value),
                contract_first(flat_upstream, flat_projected),
            ],
            axis=1,
        ).astype(jnp.bfloat16),
        "dp",
        scatter_dimension=0,
        tiled=True,
    ).astype(jnp.float32)
    token_total = lax.psum(local_count, "dp")
    scaled_grads = reduced / token_total
    grad_value = scaled_grads[:, :half_value][None]
    grad_output = scaled_grads[:, half_value:].T[None]
    return (grad_value, grad_output)


def rotate(block, axis, distance):
    count = lax.axis_size(axis)
    return lax.ppermute(block, axis, [(i, (i + distance) % count) for i in range(count)])


def swap(block, axis):
    return rotate(block, axis, 1)


PREP_LIMIT = 60 * 1024 * 1024
VMEM = pl.BlockSpec(memory_space=pltpu.VMEM)
SMEM = pl.BlockSpec(memory_space=pltpu.SMEM)
HBM = pl.BlockSpec(memory_space=pltpu.HBM)


def on_core(body, outs, operands, flops, moved, scratch=(), specs=None, limit=32 * 1024 * 1024):
    return pl.pallas_call(
        body,
        out_shape=outs,
        in_specs=[SMEM] + (specs or [VMEM] * (len(operands) - 1)),
        out_specs=[VMEM] * len(outs),
        scratch_shapes=list(scratch),
        cost_estimate=pl.CostEstimate(flops=flops, bytes_accessed=moved, transcendentals=0),
        compiler_params=pltpu.CompilerParams(vmem_limit_bytes=limit),
    )(*operands)


def shape_of(rows, cols, dtype=jnp.bfloat16):
    return jax.ShapeDtypeStruct((rows, cols), dtype)


def dot_nt(left, right):
    return lax.dot_general(
        left, right, (((1,), (1,)), ((), ())), preferred_element_type=jnp.float32
    )


def dot_nn(left, right):
    return lax.dot_general(
        left, right, (((1,), (0,)), ((), ())), preferred_element_type=jnp.float32
    )


def tile_at(index, size):
    return pl.ds(pl.multiple_of(index * size, size), size)


def fetch(pairs, sems):
    copies = [pltpu.make_async_copy(src, dst, sems.at[i]) for i, (src, dst) in enumerate(pairs)]
    for copy in copies:
        copy.start()
    return copies


def prep_body(count, place, hidden, unembed, value_proj, output_proj, gains, *refs):
    f32, bf16 = jnp.float32, jnp.bfloat16
    pieces, (ab, across, gain_out) = refs[:count], refs[count : count + 3]
    held, value_held, output_held, sems = refs[count + 3 :]
    first, dp_index, tensor_index = place[0] == 1, place[1], place[2]
    rows, width = pieces[0].shape
    half = output_proj.shape[0]
    at = tile_at(tensor_index, rows)

    def rows_from(source):
        pairs = []
        for d in range(count):
            col = tile_at(lax.rem(dp_index + d, count), width)
            pairs.append((source.at[at, col], held.at[d]))
        return [pltpu.make_async_copy(*pair, sems.at[i]) for i, pair in enumerate(pairs)]

    def start_rows(source):
        for copy in rows_from(source):
            copy.start()

    loads = [
        pltpu.make_async_copy(value_proj, value_held, sems.at[count]),
        pltpu.make_async_copy(output_proj, output_held, sems.at[count + 1]),
    ]
    for load in loads:
        load.start()
    pl.when(first)(lambda: start_rows(hidden))
    pl.when(jnp.logical_not(first))(lambda: start_rows(unembed))
    gain = gains[:, tile_at(dp_index, width)]
    gain_out[...] = gain
    loads[0].wait()
    scaled = (value_held[...].astype(f32).T * gain).astype(bf16)
    loads[1].wait()
    ab[:half, :] = scaled
    ab[half:, :] = output_held[...]
    across[...] = jnp.where(first, output_held[...], scaled)
    for d, copy in enumerate(rows_from(hidden)):
        copy.wait()
        pieces[d][...] = held[d]


def column_body(
    place, lengths, assign, survive, advantage, hidden, unembed, base, gap, cols, held, sems
):
    f32 = jnp.float32
    tensor_index = place[2]
    positions, resp_count = base.shape
    half_resp = resp_count // 2
    rows = half_resp * positions
    at = tile_at(tensor_index, rows)
    copies = fetch([(hidden.at[at], held.at[0]), (unembed.at[at], held.at[1])], sems)

    def spread(scalars):
        return jnp.concatenate([jnp.full((positions, 1), v, f32) for v in scalars], axis=0)

    def tall(array):
        both = array[...].T
        mine = jnp.where(tensor_index == 0, both[:half_resp], both[half_resp:])
        wide = jnp.concatenate(
            [jnp.broadcast_to(mine[r : r + 1, :], (positions, positions)) for r in range(half_resp)],
            axis=0,
        )
        row = lax.broadcasted_iota(jnp.int32, (rows, positions), 0)
        lane = lax.broadcasted_iota(jnp.int32, (rows, positions), 1)
        return jnp.sum(
            jnp.where(lane == lax.rem(row, positions), wide, 0.0), axis=-1, keepdims=True
        )

    here = [tensor_index * half_resp + r for r in range(half_resp)]
    listed = []
    for r in here:
        found = assign[0] == r
        for k in range(1, resp_count):
            found = found | (assign[k] == r)
        listed.append(jnp.where(found, 1.0, 0.0))
    group = resp_count // survive.shape[0]
    tokens = jnp.float32(0.0)
    for r in range(resp_count):
        tokens = tokens + (survive[r // group] * lengths[r]).astype(f32)
    listed = spread(listed)
    length = spread([lengths[r].astype(f32) for r in here])
    adv = spread([advantage[r] for r in here])
    position = lax.broadcasted_iota(jnp.int32, (rows, 1), 0)
    position = lax.rem(position, positions).astype(f32)
    gap_rows = tall(gap)
    clipped = (adv > 0) & (gap_rows > clip_high) | (adv < 0) & (gap_rows < clip_low)
    used = (position < length) & (listed > 0) & jnp.logical_not(clipped)
    weight = jnp.where(used, -loss_scale * adv, 0.0)
    for copy in copies:
        copy.wait()
    hid, un = held[0].astype(f32), held[1].astype(f32)
    square0 = jnp.sum(hid * hid, axis=-1, keepdims=True)
    dot0 = jnp.sum(hid * un, axis=-1, keepdims=True)
    lane = lax.broadcasted_iota(jnp.int32, cols.shape, 1)
    out = jnp.zeros(cols.shape, f32)
    for k, value in enumerate((square0, dot0, weight, tall(base), listed, spread([tokens] * half_resp))):
        out = jnp.where(lane == k, value, out)
    cols[...] = out


def product_body(count, place, ab, ab_other, c_own, *refs):
    first, dp_index, group_index = place[0] == 1, place[1], place[3]
    own_out, sends, scratch = refs[0], refs[1:-1], refs[-1]
    half = c_own.shape[0]
    rows = scratch.shape[0]
    at = tile_at(group_index, rows)
    low = pl.ds(half + pl.multiple_of(group_index * rows, rows), rows)
    left = jnp.where(first, ab[low, :], c_own[at, :])
    for k, source in enumerate((ab, ab_other)):
        right = jnp.where(first, source[half:, :], source[:half, :])
        scratch[:, k * half : (k + 1) * half] = dot_nt(left, right)
    step = rows // count
    own_out[...] = scratch[tile_at(dp_index, step), :]
    for d, send in enumerate(sends):
        send[...] = scratch[tile_at(lax.rem(dp_index + d + 1, count), step), :].astype(jnp.bfloat16)


def total_body(place, own, *refs):
    total = own[...]
    for ref in refs[:-1]:
        total = total + ref[...].astype(jnp.float32)
    refs[-1][...] = total.astype(jnp.bfloat16)


def order_body(count, place, *refs):
    dp_index, out = place[1], refs[-1]
    step = refs[0].shape[0]
    for d in range(count):
        out[tile_at(lax.rem(dp_index + count - d, count), step), :] = refs[d][...]


def group_body(count, place, *refs):
    group_index, out = place[3], refs[-1]
    step = refs[0].shape[0]
    for d in range(count):
        out[tile_at(lax.rem(group_index + count - d, count), step), :] = refs[d][...]


def sum_body(width, place, cols, own, *refs):
    backs, (mine, early) = refs[:-2], refs[-2:]
    total = own[...]
    for ref in backs:
        total = total + ref[...].astype(jnp.float32)
    total = total.astype(jnp.bfloat16)
    mine[...] = total
    size = early.shape[1]
    r0 = lax.rsqrt(cols[:, 0:1] / width + eps_norm)
    scaled = (r0 * total[:, :size].astype(jnp.float32)).astype(jnp.bfloat16)
    early[...] = jnp.where(place[0] == 1, scaled, total[:, size : 2 * size])


def stage_body(count, flag, *refs):
    pieces, (ab, ab_other, c_own, c_other) = refs[:count], refs[count : count + 4]
    rows_out, own_out = refs[count + 4 : count + 6]
    back_out = refs[count + 6 :]
    rows, half = pieces[0].shape[0], c_own.shape[0]
    for i, piece in enumerate(pieces):
        rows_out[i * rows : (i + 1) * rows, :] = piece[...]
    blocks = [
        (ab, 0),
        (ab_other, 0),
        (ab, half),
        (ab_other, half),
        (c_own, 0),
        (c_other, 0),
    ]
    for k, (block, start) in enumerate(blocks):
        product = dot_nt(rows_out[...], block[start : start + half, :])
        cols = slice(k * half, (k + 1) * half)
        own_out[:, cols] = product[:rows]
        for i, back in enumerate(back_out):
            back[:, cols] = product[(i + 1) * rows : (i + 2) * rows].astype(jnp.bfloat16)


def value_body(
    width, flag, mine, theirs, grown, across, grown_other, across_other, cols, late_out
):
    f32, bf16 = jnp.float32, jnp.bfloat16
    half = grown.shape[0]
    first = flag[0] == 1

    def part(own, other, index):
        at = slice(index * half, (index + 1) * half)
        return jnp.where(first, own[:, at].astype(f32), other[:, at].astype(f32))

    a0 = [part(mine, theirs, i) for i in (0, 1)]
    b0 = [part(mine, theirs, i) for i in (2, 3)]
    a1 = [part(mine, theirs, i) for i in (4, 5)]
    t1 = [part(theirs, mine, i) for i in (2, 3)]
    t0 = [part(theirs, mine, i) for i in (4, 5)]
    square0, dot0, weight = cols[:, 0:1], cols[:, 1:2], cols[:, 2:3]
    base, listed, tokens = cols[:, 3:4], cols[:, 4:5], cols[:, 5:6]

    def row_sum(pair):
        return jnp.sum(pair[0] + pair[1], axis=-1, keepdims=True)

    def square(own, other):
        return ((own[:, :half], own[:, half:]), (other[:, half:], other[:, :half]))

    gram = square(
        jnp.where(first, grown[...], across[...]), jnp.where(first, grown_other[...], across_other[...])
    )
    link = square(
        jnp.where(first, across[...], grown[...]), jnp.where(first, across_other[...], grown_other[...])
    )
    r0 = lax.rsqrt(square0 / width + eps_norm)
    p0b = [(r0 * v).astype(bf16) for v in a0]
    p0 = [v.astype(f32) for v in p0b]
    linked = [dot_nn(p0b[0], link[0][i]) + dot_nn(p0b[1], link[1][i]) for i in (0, 1)]
    low = [b0[i] + dot_nn(p0b[0], gram[0][i]) + dot_nn(p0b[1], gram[1][i]) for i in (0, 1)]
    square1 = square0 + row_sum([p0[i] * (b0[i] + low[i]) for i in (0, 1)])
    r1 = lax.rsqrt(jnp.maximum(square1, 0.0) / width + eps_norm)
    p1 = [r1 * (a1[i] + linked[i]) for i in (0, 1)]
    logit = dot0 + row_sum([p0[i] * t0[i] + p1[i] * t1[i] for i in (0, 1)])
    seed = weight * jnp.exp(jnp.where(listed > 0.0, logit - base, 0.0))
    gp1 = [seed * v for v in t1]
    c1 = r1 * r1 * row_sum([gp1[i] * p1[i] for i in (0, 1)]) / width
    gp1b = [v.astype(bf16) for v in gp1]
    back = [dot_nt(gp1b[0], link[i][0]) + dot_nt(gp1b[1], link[i][1]) for i in (0, 1)]
    gp0 = [seed * t0[i] + r1 * back[i] - c1 * low[i] for i in (0, 1)]
    late = [jnp.where(first, r0 * gp0[i], seed * p1[i]).astype(bf16) for i in (0, 1)]
    lane = lax.broadcasted_iota(jnp.int32, (mine.shape[0], 128), 1)
    extra = jnp.zeros((mine.shape[0], 128), f32)
    for k, value in enumerate((seed, r1, c1, tokens)):
        high = value.astype(bf16).astype(f32)
        extra = jnp.where(lane == k, high, jnp.where(lane == k + 4, value - high, extra))
    late_out[:, :half] = late[0]
    late_out[:, half : 2 * half] = late[1]
    late_out[:, 2 * half :] = extra.astype(bf16)


def chunk_of(width):
    return 256 if width % 256 == 0 else width


def middle_body(
    flag,
    own,
    cross,
    own_other,
    cross_other,
    early,
    early_cross,
    early_other,
    early_cross_other,
    ab,
    ab_other,
    c_own,
    c_other,
    gain,
    x1_out,
    n1_out,
    right_out,
):
    f32, bf16 = jnp.float32, jnp.bfloat16
    first = flag[0] == 1
    half, width = c_own.shape
    rows = own.shape[0]
    step = chunk_of(width)
    halves = ((own, cross, early, early_cross, 0), (own_other, cross_other, early_other, early_cross_other, 1))
    for h, (here, there, e_here, e_there, flipped) in enumerate(halves):
        p0 = jnp.where(first, e_here[...], e_there[...])
        t1 = jnp.where(first, e_there[...], e_here[...])
        mine, other = (slice(half, 2 * half), slice(0, half))[:: 1 if flipped else -1]
        at = slice(h * rows, (h + 1) * rows)
        for k in range(0, width, step):
            col = slice(k, k + step)
            wo_own = jnp.where(first, ab[half:, col], c_own[:, col])
            wo_other = jnp.where(first, ab_other[half:, col], c_other[:, col])
            hid = jnp.where(first, here[:, col], there[:, col]).astype(f32)
            x1 = hid + dot_nn(p0[:, mine], wo_own) + dot_nn(p0[:, other], wo_other)
            x1_out[at, col] = x1.astype(bf16)
            n1 = dot_nn(t1[:, mine], c_own[:, col]) + dot_nn(t1[:, other], c_other[:, col])
            n1_out[at, col] = n1.astype(bf16)
            right = jnp.where(first, hid, x1) * gain[:, col]
            right_out[col, at] = right.astype(bf16).T


def last_body(
    count,
    flag,
    *refs,
):
    f32, bf16 = jnp.float32, jnp.bfloat16
    pieces, pieces_other = refs[:count], refs[count : 2 * count]
    (own, cross, own_other, cross_other, early, early_cross, early_other, early_cross_other) = refs[
        2 * count : 2 * count + 8
    ]
    x1, n1, right, value_out, output_out, left_scr = refs[2 * count + 8 :]
    first = flag[0] == 1
    half = value_out.shape[1]
    width = right.shape[0]
    rows = own.shape[0]
    h = rows // count
    step = chunk_of(width)
    both = [*pieces, *pieces_other]
    ext = jnp.concatenate([p[:, 2 * half :] for p in both], axis=0).astype(f32)
    ext = ext[:, 0:4] + ext[:, 4:8]
    seed, r1, c1 = ext[:, 0:1], ext[:, 1:2], ext[:, 2:3]
    tokens = jnp.sum(ext[:, 3:4]) / (2.0 * h)
    scale = 1.0 / tokens
    late = jnp.concatenate(
        [p[:, :half] for p in pieces] + [p[:, half : 2 * half] for p in pieces_other], axis=0
    )
    e_here = jnp.concatenate([early[:, :half], early_other[:, half:]], axis=0)
    e_there = jnp.concatenate([early_cross[:, :half], early_cross_other[:, half:]], axis=0)
    value_left = jnp.where(first, late, (seed * r1 * e_here.astype(f32)).astype(bf16))
    left_scr[...] = jnp.where(first, e_here, late).T
    value_out[...] = dot_nn(right[...], value_left) * scale
    factor = seed * r1
    for k in range(0, width, step):
        col = slice(k, k + step)
        here = jnp.concatenate([own[:, col], own_other[:, col]], axis=0)
        there = jnp.concatenate([cross[:, col], cross_other[:, col]], axis=0)
        grad = (
            seed * there.astype(f32)
            + factor * n1[:, col].astype(f32)
            - c1 * x1[:, col].astype(f32)
        ).astype(bf16)
        output_out[:, col] = dot_nn(left_scr[...], jnp.where(first, grad, here)) * scale


def low_rank(
    hidden,
    unembed,
    value_proj,
    output_proj,
    norm_gains,
    survive,
    lengths,
    assign,
    advantage,
    reference_logit,
    recorded_gap,
):
    f32 = jnp.float32
    resp_count, positions, model_width = hidden.shape
    _, own_width, half_value = value_proj.shape
    value_width = 2 * half_value
    dp_count, group_count = lax.axis_size("dp"), lax.axis_size("groups")
    names = ("dp", "tensor", "groups")
    place = jnp.stack(
        [(lax.axis_index("section") == 0).astype(jnp.int32)] + [lax.axis_index(a) for a in names]
    )
    half_rows = resp_count // 2 * positions
    all_rows = dp_count * half_rows
    shifts = range(1, dp_count)
    hidden = hidden.reshape(resp_count * positions, model_width)
    unembed = unembed.reshape(resp_count * positions, model_width)

    def across_dp(block):
        return [block] + [rotate(block, "dp", d) for d in shifts]

    *pieces, ab, payload, gain = on_core(
        functools.partial(prep_body, dp_count),
        [shape_of(half_rows, own_width)] * dp_count
        + [
            shape_of(value_width, own_width),
            shape_of(half_value, own_width),
            shape_of(1, own_width, f32),
        ],
        [place, hidden, unembed, value_proj[0], output_proj[0], norm_gains],
        half_rows * model_width,
        8 * half_rows * model_width,
        [
            pltpu.VMEM((dp_count, half_rows, own_width), jnp.bfloat16),
            pltpu.VMEM((own_width, half_value), jnp.bfloat16),
            pltpu.VMEM((half_value, own_width), jnp.bfloat16),
            pltpu.SemaphoreType.DMA((dp_count + 2,)),
        ],
        [HBM, HBM, HBM, HBM, VMEM],
        limit=PREP_LIMIT,
    )
    c_own = swap(payload, "section")
    arrived = [pieces[0]] + [rotate(pieces[d], "dp", d) for d in shifts]
    ab_other = swap(ab, "tensor")
    c_other = swap(c_own, "tensor")
    (cols,) = on_core(
        column_body,
        [shape_of(half_rows, 128, f32)],
        [place, lengths, assign, survive, advantage, hidden, unembed, reference_logit.T, recorded_gap.T],
        half_rows * model_width,
        4 * half_rows * model_width,
        [
            pltpu.VMEM((2, half_rows, model_width), jnp.bfloat16),
            pltpu.SemaphoreType.DMA((2,)),
        ],
        [SMEM] * 4 + [HBM] * 2 + [VMEM] * 2,
        limit=PREP_LIMIT,
    )

    rows_here, summed, *backs = on_core(
        functools.partial(stage_body, dp_count),
        [shape_of(all_rows, own_width), shape_of(half_rows, 3 * value_width, f32)]
        + [shape_of(half_rows, 3 * value_width) for d in shifts],
        [place, *arrived, ab, ab_other, c_own, c_other],
        6 * all_rows * own_width * value_width,
        2 * (4 * value_width + 2 * all_rows) * own_width,
    )
    backs = [rotate(backs[d - 1], "dp", -d) for d in shifts]
    mine, early = on_core(
        functools.partial(sum_body, model_width),
        [shape_of(half_rows, 3 * value_width), shape_of(half_rows, value_width)],
        [place, cols, summed, *backs],
        9 * half_rows * value_width,
        24 * half_rows * value_width,
    )
    theirs = swap(mine, "section")

    part_rows = half_value // group_count
    block_rows = part_rows // dp_count
    own_part, *parts = on_core(
        functools.partial(product_body, dp_count),
        [shape_of(block_rows, value_width, f32)]
        + [shape_of(block_rows, value_width) for d in shifts],
        [place, ab, ab_other, c_own],
        2 * part_rows * own_width * value_width,
        4 * value_width * own_width,
        [pltpu.VMEM((part_rows, value_width), f32)],
    )
    parts = [rotate(parts[d - 1], "dp", d) for d in shifts]
    (total,) = on_core(
        total_body,
        [shape_of(block_rows, value_width)],
        [place, own_part, *parts],
        dp_count * block_rows * value_width,
        4 * dp_count * block_rows * value_width,
    )
    (product,) = on_core(
        functools.partial(order_body, dp_count),
        [shape_of(part_rows, value_width)],
        [place, *across_dp(total)],
        part_rows * value_width,
        4 * part_rows * value_width,
    )
    (grown,) = on_core(
        functools.partial(group_body, group_count),
        [shape_of(half_value, value_width)],
        [place, product]
        + [rotate(product, "groups", d) for d in range(1, group_count)],
        half_value * value_width,
        4 * half_value * value_width,
    )
    across = swap(grown, "section")
    grown_other = swap(grown, "tensor")
    across_other = swap(across, "tensor")

    early = jnp.concatenate(across_dp(early))
    early_cross = swap(early, "section")
    early_other = swap(early, "tensor")
    early_cross_other = swap(early_cross, "tensor")
    cross = swap(rows_here, "section")
    rows_other = swap(rows_here, "tensor")
    cross_other = swap(cross, "tensor")
    known = [rows_here, cross, rows_other, cross_other]
    known += [early, early_cross, early_other, early_cross_other]
    x1_rows, n1_rows, value_right = on_core(
        middle_body,
        [shape_of(2 * all_rows, own_width)] * 2 + [shape_of(own_width, 2 * all_rows)],
        [place, *known, ab, ab_other, c_own, c_other, gain],
        8 * all_rows * own_width * value_width,
        16 * all_rows * own_width,
    )

    (late,) = on_core(
        functools.partial(value_body, model_width),
        [shape_of(half_rows, value_width + 128)],
        [place, mine, theirs, grown, across, grown_other, across_other, cols],
        6 * half_rows * value_width * value_width,
        4 * value_width * value_width,
    )
    late = across_dp(late)
    late_other = [swap(piece, "tensor") for piece in late]
    grad_value, grad_output = on_core(
        functools.partial(last_body, dp_count),
        [shape_of(own_width, half_value, f32), shape_of(half_value, own_width, f32)],
        [place, *late, *late_other, *known, x1_rows, n1_rows, value_right],
        8 * all_rows * own_width * half_value,
        24 * all_rows * own_width,
        [pltpu.VMEM((half_value, 2 * all_rows), jnp.bfloat16)],
    )
    return (grad_value[None], grad_output[None])


def named(*arrays):
    return low_rank(*arrays)


def solution(mesh):
    placed = (
        P(("groups", "dp"), None, None),
        P(("groups", "dp"), None, None),
        P("section", "dp", "tensor"),
        P("section", "tensor", "dp"),
        P("section", None),
        P(("groups", "dp")),
        P(("groups", "dp")),
        P(("groups", "dp")),
        P(("groups", "dp")),
        P(("groups", "dp"), None),
        P(("groups", "dp"), None),
    )
    two_by_two = mesh.shape["section"] == 2 and mesh.shape["tensor"] == 2
    return jax.shard_map(
        named if two_by_two else general,
        mesh=mesh,
        in_specs=placed,
        out_specs=(
            P(("groups", "section"), "dp", "tensor"),
            P(("groups", "section"), "tensor", "dp"),
        ),
        check_vma=False,
    )
```

```python
import functools
import math

import jax
import jax.numpy as jnp
from jax import lax
from jax.experimental import pallas as pl
from jax.experimental.pallas import tpu as pltpu
from jax.sharding import PartitionSpec as P


GROUP = 16
MB_RESP = 8


eps_norm = 1e-06
loss_scale = 4096.0
clip_high = math.log(1.28)
clip_low = math.log(0.8)


def from_behind(block, axis, distance):
    devices = range(lax.axis_size(axis))
    route = [(i - distance, i) for i in devices if i - distance in devices]
    return lax.ppermute(block, axis, route)


def norm_forward(row_block, norm_gain):
    values = row_block.astype(jnp.float32)
    inverse = lax.rsqrt(jnp.mean(values * values, axis=-1, keepdims=True) + eps_norm)
    return (values, inverse, (values * inverse * norm_gain).astype(jnp.bfloat16))


def norm_backward(values, inverse, norm_gain, upstream):
    scaled = upstream * norm_gain
    inner_sum = jnp.sum(scaled * values, axis=-1, keepdims=True) / values.shape[-1]
    return inverse * scaled - values * (inverse * inverse * inverse) * inner_sum


def contract_last(left_rows, right_rows):
    return lax.dot_general(
        left_rows, right_rows, (((1,), (1,)), ((), ())), preferred_element_type=jnp.float32
    )


def contract_first(left_rows, right_rows):
    return lax.dot_general(
        left_rows, right_rows, (((0,), (0,)), ((), ())), preferred_element_type=jnp.float32
    )


def take_slot(slot_store, slot_index):
    return lax.dynamic_index_in_dim(slot_store, slot_index, 0, keepdims=False)


def put_slot(slot_store, new_value, slot_index, active):
    previous = take_slot(slot_store, slot_index)
    return lax.dynamic_update_index_in_dim(
        slot_store, jnp.where(active, new_value, previous), slot_index, 0
    )


def general(
    hidden,
    unembed,
    value_proj,
    output_proj,
    norm_gains,
    survive,
    lengths,
    assign,
    advantage,
    reference_logit,
    recorded_gap,
):
    resp_count = hidden.shape[0]
    positions = hidden.shape[1]
    model_width = hidden.shape[2]
    half_value = value_proj.shape[2]
    micro_count = resp_count // MB_RESP
    row_count = MB_RESP * positions
    section_count = lax.axis_size("section")
    section_index = lax.axis_index("section")
    is_last = section_index == section_count - 1
    norm_gain = norm_gains[0]
    alive_mask = jnp.repeat(survive, GROUP)
    local_count = jnp.sum((alive_mask * lengths).astype(jnp.float32))
    gathered_value, gathered_output = (
        lax.all_gather(value_proj, "dp", axis=1, tiled=True),
        lax.all_gather(output_proj, "dp", axis=2, tiled=True),
    )
    w_first = gathered_value[0]
    w_second = gathered_output[0]

    def pick(array):
        return jnp.take(array, assign, axis=0, mode="fill", fill_value=0)

    slot_hidden = pick(hidden).reshape(micro_count, row_count, model_width)
    slot_unembed = pick(unembed).reshape(micro_count, row_count, model_width)
    position_index = lax.broadcasted_iota(jnp.int32, (resp_count, positions), 1)
    live_mask = (position_index < pick(lengths)[:, None]).astype(jnp.float32)
    advantages = jnp.broadcast_to(pick(advantage)[:, None], (resp_count, positions))
    gap_rows = pick(recorded_gap)
    clipped = (advantages > 0) & (gap_rows > clip_high) | (advantages < 0) & (gap_rows < clip_low)
    kept_mask = 1.0 - clipped.astype(jnp.float32)
    weight_rows = (-loss_scale * advantages * kept_mask * live_mask).reshape(micro_count, row_count)
    logit_base = pick(reference_logit).reshape(micro_count, row_count)
    step_count = micro_count + section_count - 1
    store_in = jnp.zeros((micro_count, row_count, model_width), jnp.bfloat16)
    store_normed = jnp.zeros((micro_count, row_count, model_width), jnp.bfloat16)
    store_projected = jnp.zeros((micro_count, row_count, half_value), jnp.bfloat16)
    store_out = jnp.zeros((micro_count, row_count, model_width), jnp.bfloat16)
    arriving = jnp.zeros((row_count, model_width), jnp.bfloat16)
    for step_index in range(step_count):
        micro_index = step_index - section_index
        active = (micro_index >= 0) & (micro_index < micro_count)
        clamped = jnp.clip(micro_index, 0, micro_count - 1)
        entering = jnp.where(section_index == 0, take_slot(slot_hidden, clamped), arriving)
        values, inverse, normed = norm_forward(entering, norm_gain)
        projected = jnp.dot(normed, w_first, preferred_element_type=jnp.float32).astype(
            jnp.bfloat16
        )
        partial_out = jnp.dot(projected, w_second, preferred_element_type=jnp.float32)
        mixed_sum = lax.psum(partial_out.astype(jnp.bfloat16), "tensor").astype(jnp.float32)
        leaving = (values + mixed_sum).astype(jnp.bfloat16)
        store_in = put_slot(store_in, entering, clamped, active)
        store_normed = put_slot(store_normed, normed, clamped, active)
        store_projected = put_slot(store_projected, projected, clamped, active)
        store_out = put_slot(store_out, leaving, clamped, active)
        arriving = from_behind(leaving, "section", 1)
    store_upstream = jnp.zeros((micro_count, row_count, model_width), jnp.bfloat16)
    store_grad_value = jnp.zeros((micro_count, row_count, half_value), jnp.bfloat16)
    arriving = jnp.zeros((row_count, model_width), jnp.bfloat16)
    for step_index in range(step_count):
        micro_index = step_index - (section_count - 1 - section_index)
        active = (micro_index >= 0) & (micro_index < micro_count)
        clamped = jnp.clip(micro_index, 0, micro_count - 1)
        top_rows = take_slot(store_out, clamped).astype(jnp.float32)
        unembed_rows = take_slot(slot_unembed, clamped).astype(jnp.float32)
        logit = jnp.sum(top_rows * unembed_rows, axis=-1)
        seed_rows = take_slot(weight_rows, clamped) * jnp.exp(
            logit - take_slot(logit_base, clamped)
        )
        start_grad = (seed_rows[:, None] * unembed_rows).astype(jnp.bfloat16)
        upstream = jnp.where(is_last, start_grad, arriving)
        entering = take_slot(store_in, clamped)
        normed = take_slot(store_normed, clamped)
        projected = take_slot(store_projected, clamped)
        grad_projected = contract_last(upstream, w_second).astype(jnp.bfloat16)
        partial_norm = contract_last(grad_projected, w_first)
        grad_normed = lax.psum(partial_norm.astype(jnp.bfloat16), "tensor").astype(jnp.float32)
        values, inverse, _ = norm_forward(entering, norm_gain)
        grad_entering = (
            upstream.astype(jnp.float32) + norm_backward(values, inverse, norm_gain, grad_normed)
        ).astype(jnp.bfloat16)
        store_upstream = put_slot(store_upstream, upstream, clamped, active)
        store_grad_value = put_slot(store_grad_value, grad_projected, clamped, active)
        arriving = from_behind(grad_entering, "section", -1)
    flat_normed = store_normed.reshape(micro_count * row_count, model_width)
    flat_upstream = store_upstream.reshape(micro_count * row_count, model_width)
    flat_grad_value = store_grad_value.reshape(micro_count * row_count, half_value)
    flat_projected = store_projected.reshape(micro_count * row_count, half_value)
    reduced = lax.psum_scatter(
        jnp.concatenate(
            [
                contract_first(flat_normed, flat_grad_value),
                contract_first(flat_upstream, flat_projected),
            ],
            axis=1,
        ).astype(jnp.bfloat16),
        "dp",
        scatter_dimension=0,
        tiled=True,
    ).astype(jnp.float32)
    token_total = lax.psum(local_count, "dp")
    scaled_grads = reduced / token_total
    grad_value = scaled_grads[:, :half_value][None]
    grad_output = scaled_grads[:, half_value:].T[None]
    return (grad_value, grad_output)


def rotate(block, axis, distance):
    count = lax.axis_size(axis)
    return lax.ppermute(block, axis, [(i, (i + distance) % count) for i in range(count)])


def flip(block, bit):
    count = lax.axis_size("dp")
    return lax.ppermute(block, "dp", [(i, i ^ bit) for i in range(count)])


def low_bit(index):
    return index & -index


def sum_order(count):
    return sorted(range(1, count), key=lambda r: (low_bit(r), -r))


def swap(block, axis):
    return rotate(block, axis, 1)


VMEM = pl.BlockSpec(memory_space=pltpu.VMEM)
SMEM = pl.BlockSpec(memory_space=pltpu.SMEM)
HBM = pl.BlockSpec(memory_space=pltpu.HBM)


def on_core(body, outs, operands, flops, moved, scratch=(), specs=None, limit=32 * 1024 * 1024):
    return pl.pallas_call(
        body,
        out_shape=outs,
        in_specs=[SMEM] + (specs or [VMEM] * (len(operands) - 1)),
        out_specs=[VMEM] * len(outs),
        scratch_shapes=list(scratch),
        cost_estimate=pl.CostEstimate(flops=flops, bytes_accessed=moved, transcendentals=0),
        compiler_params=pltpu.CompilerParams(vmem_limit_bytes=limit),
    )(*operands)


def shape_of(rows, cols, dtype=jnp.bfloat16):
    return jax.ShapeDtypeStruct((rows, cols), dtype)


def dot_nt(left, right):
    return lax.dot_general(
        left, right, (((1,), (1,)), ((), ())), preferred_element_type=jnp.float32
    )


def dot_nn(left, right):
    return lax.dot_general(
        left, right, (((1,), (0,)), ((), ())), preferred_element_type=jnp.float32
    )


def tile_at(index, size):
    return pl.ds(pl.multiple_of(index * size, size), size)


def fetch(pairs, sems):
    copies = [pltpu.make_async_copy(src, dst, sems.at[i]) for i, (src, dst) in enumerate(pairs)]
    for copy in copies:
        copy.start()
    return copies


def scaled_to(out, held, gain):
    _, width = out.shape
    step = width // 2 if width % 256 == 0 else width
    for k in range(0, width, step):
        block = held[k : k + step, :].astype(jnp.float32).T
        out[:, k : k + step] = (block * gain[:, k : k + step]).astype(jnp.bfloat16)


def own_body(place, value_proj, output_proj, gain, ab):
    half, _ = output_proj.shape
    scaled_to(ab.at[:half], value_proj, gain)
    ab[half:, :] = output_proj[...]


def column_body(
    place, lengths, assign, survive, advantage, hidden, unembed, base, gap, cols, held, sems
):
    f32 = jnp.float32
    tensor_index = place[2]
    positions, resp_count = base.shape
    half_resp = resp_count // 2
    rows = half_resp * positions
    at = tile_at(tensor_index, rows)
    copies = fetch([(hidden.at[at], held.at[0]), (unembed.at[at], held.at[1])], sems)

    def spread(scalars):
        return jnp.concatenate([jnp.full((positions, 1), v, f32) for v in scalars], axis=0)

    def tall(array):
        both = array[...].T
        mine = jnp.where(tensor_index == 0, both[:half_resp], both[half_resp:])
        wide = jnp.concatenate(
            [jnp.broadcast_to(mine[r : r + 1, :], (positions, positions)) for r in range(half_resp)],
            axis=0,
        )
        row = lax.broadcasted_iota(jnp.int32, (rows, positions), 0)
        lane = lax.broadcasted_iota(jnp.int32, (rows, positions), 1)
        return jnp.sum(
            jnp.where(lane == lax.rem(row, positions), wide, 0.0), axis=-1, keepdims=True
        )

    here = [tensor_index * half_resp + r for r in range(half_resp)]
    listed = []
    for r in here:
        found = assign[0] == r
        for k in range(1, resp_count):
            found = found | (assign[k] == r)
        listed.append(jnp.where(found, 1.0, 0.0))
    group = resp_count // survive.shape[0]
    tokens = jnp.float32(0.0)
    for r in range(resp_count):
        tokens = tokens + (survive[r // group] * lengths[r]).astype(f32)
    listed = spread(listed)
    length = spread([lengths[r].astype(f32) for r in here])
    adv = spread([advantage[r] for r in here])
    position = lax.broadcasted_iota(jnp.int32, (rows, 1), 0)
    position = lax.rem(position, positions).astype(f32)
    gap_rows = tall(gap)
    clipped = (adv > 0) & (gap_rows > clip_high) | (adv < 0) & (gap_rows < clip_low)
    used = (position < length) & (listed > 0) & jnp.logical_not(clipped)
    weight = jnp.where(used, -loss_scale * adv, 0.0)
    for copy in copies:
        copy.wait()
    hid, un = held[0].astype(f32), held[1].astype(f32)
    square0 = jnp.sum(hid * hid, axis=-1, keepdims=True)
    dot0 = jnp.sum(hid * un, axis=-1, keepdims=True)
    lane = lax.broadcasted_iota(jnp.int32, cols.shape, 1)
    out = jnp.zeros(cols.shape, f32)
    for k, value in enumerate((square0, dot0, weight, tall(base), listed, spread([tokens] * half_resp))):
        out = jnp.where(lane == k, value, out)
    cols[...] = out


def product_body(place, ab, ab_other, c_own, own_out, send_out):
    first, group_index = place[0] == 1, place[3]
    half = c_own.shape[0]
    rows = own_out.shape[0]
    low = pl.ds(half + pl.multiple_of(group_index * rows, rows), rows)
    left = jnp.where(first, ab[low, :], c_own[tile_at(group_index, rows), :])
    for k, source in enumerate((ab, ab_other)):
        right = jnp.where(first, source[half:, :], source[:half, :])
        product = dot_nt(left, right)
        own_out[:, k * half : (k + 1) * half] = product
        send_out[:, k * half : (k + 1) * half] = product.astype(jnp.bfloat16)


def add_body(place, own, *refs):
    total = own[...]
    for ref in refs[:-1]:
        total = total + ref[...].astype(jnp.float32)
    refs[-1][...] = total.astype(jnp.bfloat16)


def total_body(place, own, other, total_out, send_out):
    total = own[...] + other[...].astype(jnp.float32)
    total_out[...] = total
    send_out[...] = total.astype(jnp.bfloat16)


def group_body(count, place, *refs):
    group_index, out = place[3], refs[-1]
    step = refs[0].shape[0]
    for d in range(count):
        out[tile_at(lax.rem(group_index + count - d, count), step), :] = refs[d][...]


def sum_body(width, place, cols, own, *refs):
    backs, (mine, early) = refs[:-2], refs[-2:]
    total = own[...]
    for ref in backs:
        total = total + ref[...].astype(jnp.float32)
    total = total.astype(jnp.bfloat16)
    mine[...] = total
    size = early.shape[1]
    r0 = lax.rsqrt(cols[:, 0:1] / width + eps_norm)
    scaled = (r0 * total[:, :size].astype(jnp.float32)).astype(jnp.bfloat16)
    early[...] = jnp.where(place[0] == 1, scaled, total[:, size : 2 * size])


def stage_body(count, flag, *refs):
    pieces, (ab, ab_other, c_own, c_other) = refs[:count], refs[count : count + 4]
    rows_out, back_out = refs[count + 4], refs[count + 5 :]
    rows, half = pieces[0].shape[0], c_own.shape[0]
    for i, piece in enumerate(pieces):
        rows_out[i * rows : (i + 1) * rows, :] = piece[...]
    blocks = [
        (ab, 0),
        (ab_other, 0),
        (ab, half),
        (ab_other, half),
        (c_own, 0),
        (c_other, 0),
    ]
    for k, (block, start) in enumerate(blocks):
        product = dot_nt(rows_out[...], block[start : start + half, :])
        cols = slice(k * half, (k + 1) * half)
        for i, back in enumerate(back_out):
            back[:, cols] = product[i * rows : (i + 1) * rows].astype(back.dtype)


def value_body(
    width, flag, mine, theirs, grown, across, grown_other, across_other, cols, late_out
):
    f32, bf16 = jnp.float32, jnp.bfloat16
    half = grown.shape[0]
    first = flag[0] == 1

    def part(own, other, index):
        at = slice(index * half, (index + 1) * half)
        return jnp.where(first, own[:, at].astype(f32), other[:, at].astype(f32))

    a0 = [part(mine, theirs, i) for i in (0, 1)]
    b0 = [part(mine, theirs, i) for i in (2, 3)]
    a1 = [part(mine, theirs, i) for i in (4, 5)]
    t1 = [part(theirs, mine, i) for i in (2, 3)]
    t0 = [part(theirs, mine, i) for i in (4, 5)]
    square0, dot0, weight = cols[:, 0:1], cols[:, 1:2], cols[:, 2:3]
    base, listed, tokens = cols[:, 3:4], cols[:, 4:5], cols[:, 5:6]

    def row_sum(pair):
        return jnp.sum(pair[0] + pair[1], axis=-1, keepdims=True)

    def square(own, other):
        return ((own[:, :half], own[:, half:]), (other[:, half:], other[:, :half]))

    gram = square(
        jnp.where(first, grown[...], across[...]), jnp.where(first, grown_other[...], across_other[...])
    )
    link = square(
        jnp.where(first, across[...], grown[...]), jnp.where(first, across_other[...], grown_other[...])
    )
    r0 = lax.rsqrt(square0 / width + eps_norm)
    p0b = [(r0 * v).astype(bf16) for v in a0]
    p0 = [v.astype(f32) for v in p0b]
    linked = [dot_nn(p0b[0], link[0][i]) + dot_nn(p0b[1], link[1][i]) for i in (0, 1)]
    low = [b0[i] + dot_nn(p0b[0], gram[0][i]) + dot_nn(p0b[1], gram[1][i]) for i in (0, 1)]
    square1 = square0 + row_sum([p0[i] * (b0[i] + low[i]) for i in (0, 1)])
    r1 = lax.rsqrt(jnp.maximum(square1, 0.0) / width + eps_norm)
    p1 = [r1 * (a1[i] + linked[i]) for i in (0, 1)]
    logit = dot0 + row_sum([p0[i] * t0[i] + p1[i] * t1[i] for i in (0, 1)])
    seed = weight * jnp.exp(jnp.where(listed > 0.0, logit - base, 0.0))
    gp1 = [seed * v for v in t1]
    c1 = r1 * r1 * row_sum([gp1[i] * p1[i] for i in (0, 1)]) / width
    gp1b = [v.astype(bf16) for v in gp1]
    back = [dot_nt(gp1b[0], link[i][0]) + dot_nt(gp1b[1], link[i][1]) for i in (0, 1)]
    gp0 = [seed * t0[i] + r1 * back[i] - c1 * low[i] for i in (0, 1)]
    late = [jnp.where(first, r0 * gp0[i], seed * p1[i]).astype(bf16) for i in (0, 1)]
    lane = lax.broadcasted_iota(jnp.int32, (mine.shape[0], 128), 1)
    extra = jnp.zeros((mine.shape[0], 128), f32)
    for k, value in enumerate((seed, r1, c1, tokens)):
        high = value.astype(bf16).astype(f32)
        extra = jnp.where(lane == k, high, jnp.where(lane == k + 4, value - high, extra))
    late_out[:, :half] = late[0]
    late_out[:, half : 2 * half] = late[1]
    late_out[:, 2 * half :] = extra.astype(bf16)


def chunk_of(width):
    return 256 if width % 256 == 0 else width


def middle_body(
    flag,
    own,
    cross,
    own_other,
    cross_other,
    early,
    early_cross,
    early_other,
    early_cross_other,
    ab,
    ab_other,
    c_own,
    c_other,
    gain,
    x1_out,
    n1_out,
    right_out,
):
    f32, bf16 = jnp.float32, jnp.bfloat16
    first = flag[0] == 1
    half, width = c_own.shape
    rows = own.shape[0]
    step = chunk_of(width)
    halves = ((own, cross, early, early_cross, 0), (own_other, cross_other, early_other, early_cross_other, 1))
    for h, (here, there, e_here, e_there, flipped) in enumerate(halves):
        p0 = jnp.where(first, e_here[...], e_there[...])
        t1 = jnp.where(first, e_there[...], e_here[...])
        mine, other = (slice(half, 2 * half), slice(0, half))[:: 1 if flipped else -1]
        at = slice(h * rows, (h + 1) * rows)
        for k in range(0, width, step):
            col = slice(k, k + step)
            wo_own = jnp.where(first, ab[half:, col], c_own[:, col])
            wo_other = jnp.where(first, ab_other[half:, col], c_other[:, col])
            hid = jnp.where(first, here[:, col], there[:, col]).astype(f32)
            x1 = hid + dot_nn(p0[:, mine], wo_own) + dot_nn(p0[:, other], wo_other)
            x1_out[at, col] = x1.astype(bf16)
            n1 = dot_nn(t1[:, mine], c_own[:, col]) + dot_nn(t1[:, other], c_other[:, col])
            n1_out[at, col] = n1.astype(bf16)
            right = jnp.where(first, hid, x1) * gain[:, col]
            right_out[col, at] = right.astype(bf16).T


def last_body(
    count,
    flag,
    *refs,
):
    f32, bf16 = jnp.float32, jnp.bfloat16
    pieces, pieces_other = refs[:count], refs[count : 2 * count]
    (own, cross, own_other, cross_other, early, early_cross, early_other, early_cross_other) = refs[
        2 * count : 2 * count + 8
    ]
    x1, n1, right, value_out, output_out, left_scr = refs[2 * count + 8 :]
    first = flag[0] == 1
    half = value_out.shape[1]
    width = right.shape[0]
    rows = own.shape[0]
    h = rows // count
    step = chunk_of(width)
    both = [*pieces, *pieces_other]
    ext = jnp.concatenate([p[:, 2 * half :] for p in both], axis=0).astype(f32)
    ext = ext[:, 0:4] + ext[:, 4:8]
    seed, r1, c1 = ext[:, 0:1], ext[:, 1:2], ext[:, 2:3]
    tokens = jnp.sum(ext[:, 3:4]) / (2.0 * h)
    scale = 1.0 / tokens
    late = jnp.concatenate(
        [p[:, :half] for p in pieces] + [p[:, half : 2 * half] for p in pieces_other], axis=0
    )
    e_here = jnp.concatenate([early[:, :half], early_other[:, half:]], axis=0)
    e_there = jnp.concatenate([early_cross[:, :half], early_cross_other[:, half:]], axis=0)
    value_left = jnp.where(first, late, (seed * r1 * e_here.astype(f32)).astype(bf16))
    left_scr[...] = jnp.where(first, e_here, late).T
    value_out[...] = dot_nn(right[...], value_left) * scale
    factor = seed * r1
    for k in range(0, width, step):
        col = slice(k, k + step)
        here = jnp.concatenate([own[:, col], own_other[:, col]], axis=0)
        there = jnp.concatenate([cross[:, col], cross_other[:, col]], axis=0)
        grad = (
            seed * there.astype(f32)
            + factor * n1[:, col].astype(f32)
            - c1 * x1[:, col].astype(f32)
        ).astype(bf16)
        output_out[:, col] = dot_nn(left_scr[...], jnp.where(first, grad, here)) * scale


def low_rank(
    hidden,
    unembed,
    value_proj,
    output_proj,
    norm_gains,
    survive,
    lengths,
    assign,
    advantage,
    reference_logit,
    recorded_gap,
):
    f32 = jnp.float32
    resp_count, positions, model_width = hidden.shape
    _, own_width, half_value = value_proj.shape
    value_width = 2 * half_value
    dp_count, group_count = lax.axis_size("dp"), lax.axis_size("groups")
    names = ("dp", "tensor", "groups")
    place = jnp.stack(
        [(lax.axis_index("section") == 0).astype(jnp.int32)] + [lax.axis_index(a) for a in names]
    )
    half_rows = resp_count // 2 * positions
    all_rows = dp_count * half_rows
    shifts = range(1, dp_count)
    hidden = hidden.reshape(resp_count * positions, model_width)
    unembed = unembed.reshape(resp_count * positions, model_width)

    def across_dp(block):
        held, bit = {0: block}, dp_count // 2
        while bit:
            for r in sorted(held):
                held[r ^ bit] = flip(held[r], bit)
            bit //= 2
        return [held[r] for r in range(dp_count)]

    first = lax.axis_index("section") == 0
    dp_index = lax.axis_index("dp")
    gain = lax.dynamic_slice_in_dim(norm_gains, dp_index * own_width, own_width, 1)
    held = lax.optimization_barrier(value_proj)
    payload = jnp.where(
        first,
        output_proj[0],
        (held[0].astype(f32) * gain[0][:, None]).astype(jnp.bfloat16).T,
    )

    def piece(r):
        at = (lax.axis_index("tensor") * half_rows, (dp_index ^ r) * own_width)
        taken = [lax.dynamic_slice(a, at, (half_rows, own_width)) for a in (hidden, unembed)]
        return jnp.where(first, *taken)

    pieces = [piece(r) for r in range(dp_count)]
    pieces, hidden, unembed, value_proj, output_proj = lax.optimization_barrier(
        (pieces, hidden, unembed, value_proj, output_proj)
    )
    c_own = swap(payload, "section")
    arrived = [pieces[0]] + [flip(pieces[r], r) for r in shifts]
    (ab,) = on_core(
        own_body,
        [shape_of(value_width, own_width)],
        [place, value_proj[0], output_proj[0], gain],
        half_value * own_width,
        8 * half_value * own_width,
    )
    ab_other = swap(ab, "tensor")
    c_other = swap(c_own, "tensor")
    (cols,) = on_core(
        column_body,
        [shape_of(half_rows, 128, f32)],
        [place, lengths, assign, survive, advantage, hidden, unembed, reference_logit.T, recorded_gap.T],
        half_rows * model_width,
        4 * half_rows * model_width,
        [
            pltpu.VMEM((2, half_rows, model_width), jnp.bfloat16),
            pltpu.SemaphoreType.DMA((2,)),
        ],
        [SMEM] * 4 + [HBM] * 2 + [VMEM] * 2,
    )

    rows_here, *sums = on_core(
        functools.partial(stage_body, dp_count),
        [shape_of(all_rows, own_width)]
        + [
            shape_of(half_rows, 3 * value_width, jnp.bfloat16 if r % 2 else f32)
            for r in range(dp_count)
        ],
        [place, *arrived, ab, ab_other, c_own, c_other],
        6 * all_rows * own_width * value_width,
        2 * (4 * value_width + 2 * all_rows) * own_width,
    )
    got = {r: [] for r in range(dp_count)}
    for r in sum_order(dp_count):
        sent = sums[r]
        if got[r]:
            (sent,) = on_core(
                add_body,
                [shape_of(half_rows, 3 * value_width)],
                [place, sent, *got[r]],
                3 * half_rows * value_width,
                24 * half_rows * value_width,
            )
        got[r ^ low_bit(r)].append(flip(sent, low_bit(r)))
    mine, early = on_core(
        functools.partial(sum_body, model_width),
        [shape_of(half_rows, 3 * value_width), shape_of(half_rows, value_width)],
        [place, cols, sums[0], *got[0]],
        9 * half_rows * value_width,
        24 * half_rows * value_width,
    )
    theirs = swap(mine, "section")

    part_rows = half_value // group_count
    part_shapes = [shape_of(part_rows, value_width, f32), shape_of(part_rows, value_width)]
    part, product = on_core(
        product_body,
        part_shapes,
        [place, ab, ab_other, c_own],
        2 * part_rows * own_width * value_width,
        4 * value_width * own_width,
    )
    step = 1
    while step < dp_count:
        other = flip(product, step)
        last = 2 * step >= dp_count
        *kept, product = on_core(
            add_body if last else total_body,
            part_shapes[1:] if last else part_shapes,
            [place, part, other],
            part_rows * value_width,
            12 * part_rows * value_width,
        )
        part = None if last else kept[0]
        step *= 2
    (grown,) = on_core(
        functools.partial(group_body, group_count),
        [shape_of(half_value, value_width)],
        [place, product]
        + [rotate(product, "groups", d) for d in range(1, group_count)],
        half_value * value_width,
        4 * half_value * value_width,
    )
    across = swap(grown, "section")
    grown_other = swap(grown, "tensor")
    across_other = swap(across, "tensor")

    early = jnp.concatenate(across_dp(early))
    early_cross = swap(early, "section")
    early_other = swap(early, "tensor")
    early_cross_other = swap(early_cross, "tensor")
    cross = swap(rows_here, "section")
    rows_other = swap(rows_here, "tensor")
    cross_other = swap(cross, "tensor")
    known = [rows_here, cross, rows_other, cross_other]
    known += [early, early_cross, early_other, early_cross_other]
    x1_rows, n1_rows, value_right = on_core(
        middle_body,
        [shape_of(2 * all_rows, own_width)] * 2 + [shape_of(own_width, 2 * all_rows)],
        [place, *known, ab, ab_other, c_own, c_other, gain],
        8 * all_rows * own_width * value_width,
        16 * all_rows * own_width,
    )

    (late,) = on_core(
        functools.partial(value_body, model_width),
        [shape_of(half_rows, value_width + 128)],
        [place, mine, theirs, grown, across, grown_other, across_other, cols],
        6 * half_rows * value_width * value_width,
        4 * value_width * value_width,
    )
    late = across_dp(late)
    late_other = [swap(piece, "tensor") for piece in late]
    grad_value, grad_output = on_core(
        functools.partial(last_body, dp_count),
        [shape_of(own_width, half_value, f32), shape_of(half_value, own_width, f32)],
        [place, *late, *late_other, *known, x1_rows, n1_rows, value_right],
        8 * all_rows * own_width * half_value,
        24 * all_rows * own_width,
        [pltpu.VMEM((half_value, 2 * all_rows), jnp.bfloat16)],
    )
    return (grad_value[None], grad_output[None])


def named(*arrays):
    return low_rank(*arrays)


def solution(mesh):
    placed = (
        P(("groups", "dp"), None, None),
        P(("groups", "dp"), None, None),
        P("section", "dp", "tensor"),
        P("section", "tensor", "dp"),
        P("section", None),
        P(("groups", "dp")),
        P(("groups", "dp")),
        P(("groups", "dp")),
        P(("groups", "dp")),
        P(("groups", "dp"), None),
        P(("groups", "dp"), None),
    )
    count = mesh.shape["dp"]
    two_by_two = mesh.shape["section"] == 2 and mesh.shape["tensor"] == 2
    two_by_two = two_by_two and count & (count - 1) == 0
    return jax.shard_map(
        named if two_by_two else general,
        mesh=mesh,
        in_specs=placed,
        out_specs=(
            P(("groups", "section"), "dp", "tensor"),
            P(("groups", "section"), "tensor", "dp"),
        ),
        check_vma=False,
    )
```
